32 devices in a mesh: rows: 32 (over z, y, x, core).
Axes of the slice: x: 2, y: 2, z: 4, core: 2. Of those that a mesh axis runs over, the one named last changes fastest.
Arguments:
- band_lower: float32 [512, 128, 128], P('rows'), may hold values from -1.1 to 0.15, as said below
- band_diag: float32 [512, 128, 128], P('rows'), may hold values from -0.3 to 5.3
- band_upper: float32 [512, 128, 128], P('rows'), may hold values from -0.15 to 1.1, as said below
- fac_lower: float32 [512, 128, 128], P('rows'), may hold values from -1 to 0.1
- pivot_inverse: float32 [512, 128, 128], P('rows'), may hold values from -0.08 to 1.08
- rhs: float32 [128, 65536], P(None, 'rows'), may hold values from -150 to 150
- start: float32 [128, 65536], P(None, 'rows'), may hold values from -0.6 to 0.6
Outputs:
- solution: float32 [128, 65536], P(None, 'rows')
- krylov: float32 [4, 128, 65536], P(None, None, 'rows')
- hessenberg: float32 [4, 3, 128], replicated
The draws below stay inside these ranges and needn't reach their ends.
Inputs may be any that keep to these rules, and one draw needn't show every extreme that they name: `band_lower`: each block is zero below its diagonal, so the band reaches 128 diagonals on each side of the main one. `band_upper`: each block is zero above its diagonal.
All inputs are finite; a program needn't handle non-finite values.
Results may differ from the reference program's by a relative error of at most 0.00024.
Values sent between devices are 32-bit elements; how exact they have to be, the bound alone decides.
A program may use at most 128 MiB of HBM per device.

```python
import math
import jax
import jax.numpy as jnp
from jax import lax

B = 128
BLK_DEV = 16
SYSTEMS = 128
ITERS = 3
NBLK = 512
ORDER = 65536
N_ROWS = 32


def banded_values(key, spread):
    values = jnp.clip(jax.random.normal(key, (NBLK, B, B), jnp.float32), -5.0, 5.0)
    return values * spread


def diagonal_blocks(key, low_value, high_value):
    entries = jax.random.uniform(key, (NBLK, B), jnp.float32, low_value, high_value)
    return jnp.eye(B, dtype=jnp.float32)[None] * entries[:, :, None]


def draw_band_lower(key, part):
    values = banded_values(jax.random.fold_in(key, 11), 0.03)
    row_index = jnp.arange(B)[:, None]
    col_index = jnp.arange(B)[None, :]
    masked = jnp.where((col_index >= row_index)[None], values, 0.0)
    return masked - diagonal_blocks(jax.random.fold_in(key, 31), 0.75, 0.95)


def draw_band_upper(key, part):
    values = banded_values(jax.random.fold_in(key, 12), 0.03)
    row_index = jnp.arange(B)[:, None]
    col_index = jnp.arange(B)[None, :]
    masked = jnp.where((col_index <= row_index)[None], values, 0.0)
    return masked + diagonal_blocks(jax.random.fold_in(key, 32), 0.75, 0.95)


def draw_band_diag(key, part):
    scattered = banded_values(jax.random.fold_in(key, 13), 0.06)
    diagonal_part = jax.random.uniform(jax.random.fold_in(key, 14), (NBLK, B), jnp.float32, 3.0, 5.0)
    return scattered + jnp.eye(B, dtype=jnp.float32)[None] * diagonal_part[:, :, None]


def draw_fac_lower(key, part):
    scattered = banded_values(jax.random.fold_in(key, 17), 0.02)
    return scattered - diagonal_blocks(jax.random.fold_in(key, 18), 0.7, 0.9)


def draw_pivot_inverse(key, part):
    scattered = banded_values(jax.random.fold_in(key, 15), 0.016)
    return scattered + diagonal_blocks(jax.random.fold_in(key, 16), 0.8, 1.0)


def draw_rhs(key, part):
    key_noise = jax.random.fold_in(key, 21)
    key_scale = jax.random.fold_in(key, 22)
    scales = jnp.exp(jax.random.uniform(key_scale, (NBLK,), jnp.float32, 0.0, math.log(10.0)))
    growth = jnp.exp(math.log(3.0) * jnp.arange(ORDER, dtype=jnp.float32) / ORDER)
    profile = jnp.repeat(scales, B, total_repeat_length=ORDER) * growth
    values = jnp.clip(jax.random.normal(key_noise, (SYSTEMS, ORDER), jnp.float32), -5.0, 5.0)
    return values * profile[None, :]


def level_of(key, shape, cuts, smallest, largest):
    level = 1.0
    for dim, blocks in cuts:
        heights = jax.random.uniform(jax.random.fold_in(jax.random.fold_in(key, 6), dim), (blocks,), jnp.float32, smallest / len(cuts), largest / len(cuts))
        level = level * jnp.repeat(jnp.exp(heights), shape[dim] // blocks).reshape((-1,) + (1,) * (len(shape) - 1 - dim))
    return level


def centred(stream_key, dims, scale, most, split=(), kind=jnp.bfloat16):
    values = scale * jax.random.normal(stream_key, dims, jnp.float32)
    if split:
        values = values * level_of(stream_key, dims, split, -0.22, 0.18)
    return jnp.clip(values, -most, most).astype(kind)


def setup_inputs(seed: int = 0) -> dict:
    key_list = jax.random.split(jax.random.key(seed), 8)
    band_lower = draw_band_lower(jax.random.fold_in(key_list[7], 71), 0)
    band_diag = draw_band_diag(jax.random.fold_in(key_list[7], 71), 0)
    band_upper = draw_band_upper(jax.random.fold_in(key_list[7], 71), 0)
    fac_lower = draw_fac_lower(jax.random.fold_in(key_list[7], 71), 0)
    pivot_inverse = draw_pivot_inverse(jax.random.fold_in(key_list[7], 71), 0)
    rhs = draw_rhs(jax.random.fold_in(key_list[7], 71), 0)
    start = centred(key_list[6], (SYSTEMS, ORDER), 0.1, 0.6, ((1, 32),), jnp.float32)
    return dict(band_lower=band_lower, band_diag=band_diag, band_upper=band_upper, fac_lower=fac_lower, pivot_inverse=pivot_inverse, rhs=rhs, start=start)


highest = lax.Precision.HIGHEST
epsilon = 1e-06

def block_apply(matrices, vectors):
    return jnp.einsum('...ij,c...j->c...i', matrices, vectors, precision=highest)

def local_solve(source, fac_lower, pivot_inverse, band_upper):
    length = source.shape[-2]
    forward = [source[..., 0, :]]
    for position in range(1, length):
        forward.append(source[..., position, :] - block_apply(fac_lower[..., position, :, :], forward[-1]))
    backward = [block_apply(pivot_inverse[..., length - 1, :, :], forward[-1])]
    for position in range(length - 2, -1, -1):
        remainder = forward[position] - block_apply(band_upper[..., position, :, :], backward[-1])
        backward.append(block_apply(pivot_inverse[..., position, :, :], remainder))
    return jnp.stack(backward[::-1], axis=-2)

def least_squares(hessenberg, start_norm):
    columns_total = hessenberg.shape[1]
    matrix = [[hessenberg[row_pos, col_pos] for col_pos in range(columns_total)] for row_pos in range(columns_total + 1)]
    target = [start_norm] + [jnp.zeros_like(start_norm) for row_pos in range(columns_total)]
    cos_terms = []
    sin_terms = []
    for col_pos in range(columns_total):
        for row_pos in range(col_pos):
            upper_entry = matrix[row_pos][col_pos]
            lower_entry = matrix[row_pos + 1][col_pos]
            matrix[row_pos][col_pos] = cos_terms[row_pos] * upper_entry + sin_terms[row_pos] * lower_entry
            matrix[row_pos + 1][col_pos] = cos_terms[row_pos] * lower_entry - sin_terms[row_pos] * upper_entry
        upper_entry = matrix[col_pos][col_pos]
        lower_entry = matrix[col_pos + 1][col_pos]
        radius = jnp.sqrt(upper_entry * upper_entry + lower_entry * lower_entry)
        cos_terms.append(upper_entry / radius)
        sin_terms.append(lower_entry / radius)
        matrix[col_pos][col_pos] = radius
        target[col_pos + 1] = -sin_terms[col_pos] * target[col_pos]
        target[col_pos] = cos_terms[col_pos] * target[col_pos]
    weights = [None] * columns_total
    for row_pos in range(columns_total - 1, -1, -1):
        partial_sum = target[row_pos]
        for col_pos in range(row_pos + 1, columns_total):
            partial_sum = partial_sum - matrix[row_pos][col_pos] * weights[col_pos]
        weights[row_pos] = partial_sum / matrix[row_pos][row_pos]
    return weights

def reference(band_lower, band_diag, band_upper, fac_lower, pivot_inverse, rhs, start):
    systems = rhs.shape[0]
    total_blocks = band_diag.shape[0]

    def apply_matrix(field):
        preceding = jnp.pad(field[:, :-1], ((0, 0), (1, 0), (0, 0)))
        following = jnp.pad(field[:, 1:], ((0, 0), (0, 1), (0, 0)))
        return block_apply(band_diag, field) + block_apply(band_lower, preceding) + block_apply(band_upper, following)
    lower_parts = band_lower.reshape(N_ROWS, BLK_DEV, B, B)
    upper_parts = band_upper.reshape(N_ROWS, BLK_DEV, B, B)
    factor_parts = fac_lower.reshape(N_ROWS, BLK_DEV, B, B)
    pivot_parts = pivot_inverse.reshape(N_ROWS, BLK_DEV, B, B)
    zero_blocks = jnp.zeros((B, N_ROWS, BLK_DEV - 1, B), jnp.float32)
    left_source = jnp.concatenate([jnp.transpose(lower_parts[:, 0], (2, 0, 1))[:, :, None, :], zero_blocks], axis=2)
    right_source = jnp.concatenate([zero_blocks, jnp.transpose(upper_parts[:, -1], (2, 0, 1))[:, :, None, :]], axis=2)
    left_spike = local_solve(left_source, factor_parts, pivot_parts, upper_parts)
    right_spike = local_solve(right_source, factor_parts, pivot_parts, upper_parts)
    top_tips = jnp.transpose(left_spike[:, :, 0, :], (1, 2, 0))
    bottom_tips = jnp.transpose(right_spike[:, :, -1, :], (1, 2, 0))
    prev_bottom = jnp.concatenate([jnp.zeros((1, B, B), jnp.float32), bottom_tips[:-1]], axis=0)
    coupling = jnp.eye(B, dtype=jnp.float32)[None] - jnp.einsum('pij,pjk->pik', top_tips, prev_bottom, precision=highest)

    def precondition(field):
        solved_local = local_solve(field.reshape(systems, N_ROWS, BLK_DEV, B), factor_parts, pivot_parts, upper_parts)
        top_values = solved_local[:, :, 0, :]
        bottom_values = solved_local[:, :, -1, :]
        prev_values = jnp.pad(bottom_values[:, :-1], ((0, 0), (1, 0), (0, 0)))
        tip_source = top_values - block_apply(top_tips, prev_values)
        top_solved = jnp.transpose(jnp.linalg.solve(coupling, jnp.transpose(tip_source, (1, 2, 0))), (2, 0, 1))
        bottom_solved = prev_values - block_apply(prev_bottom, top_solved)
        next_solved = jnp.pad(top_solved[:, 1:], ((0, 0), (0, 1), (0, 0)))
        result = solved_local - jnp.einsum('cpki,spc->spki', right_spike, next_solved, precision=highest)
        result = result - jnp.einsum('cpki,spc->spki', left_spike, bottom_solved, precision=highest)
        return result.reshape(systems, total_blocks, B)
    fields = rhs.reshape(systems, total_blocks, B)
    start_blocks = start.reshape(systems, total_blocks, B)
    residual = fields - apply_matrix(start_blocks)
    start_norm = jnp.sqrt(lax.optimization_barrier(jnp.sum(residual * residual, axis=(1, 2))) + epsilon)
    krylov = [residual / start_norm[:, None, None]]
    columns = []
    for column in range(ITERS):
        mapped = apply_matrix(precondition(krylov[column]))
        products = [lax.optimization_barrier(jnp.sum(mapped * vector, axis=(1, 2))) for vector in krylov]
        update = mapped
        for weight, vector in zip(products, krylov):
            update = update - weight[:, None, None] * vector
        length_now = jnp.sqrt(lax.optimization_barrier(jnp.sum(update * update, axis=(1, 2))) + epsilon)
        krylov.append(update / length_now[:, None, None])
        columns.append(jnp.stack(products + [length_now] + [jnp.zeros_like(start_norm)] * (ITERS - 1 - column), axis=0))
    hessenberg = jnp.stack(columns, axis=1)
    weights = least_squares(hessenberg, start_norm)
    combined = weights[0][:, None, None] * krylov[0]
    for column in range(1, ITERS):
        combined = combined + weights[column][:, None, None] * krylov[column]
    solution = start_blocks + precondition(combined)
    return (solution.reshape(systems, -1), jnp.stack(krylov).reshape(ITERS + 1, systems, -1), hessenberg)
```

```python
import jax
import jax.numpy as jnp
from jax import lax
from jax.experimental import pallas as pl
from jax.experimental.pallas import tpu as pltpu
from jax.sharding import PartitionSpec as P

ITERS = 3
EPS = 1e-06
F32, BF16 = jnp.float32, jnp.bfloat16
HIGHEST = lax.Precision.HIGHEST


def split(x):
    hi = x.astype(BF16)
    return hi, (x - hi.astype(F32)).astype(BF16)


def row(mt):
    return jnp.concatenate(split(mt), axis=1)


def mm(parts, g):
    halves = [split(part) for part in parts]
    lhs = jnp.concatenate([h for h, _ in halves] + [l for _, l in halves], axis=1)
    out = jnp.dot(lhs, jnp.concatenate([g, g], axis=0), preferred_element_type=F32)
    width = out.shape[1] // 2
    return out[:, :width] + out[:, width:]


def local_solve(f_ref, g_ref, gl, ge, gp, n, b):
    z = f_ref[:, 0:b]
    for k in range(n):
        if k:
            z = f_ref[:, k * b : (k + 1) * b] - mm([z], gl[k])
        g_ref[:, k * b : (k + 1) * b] = mm([z], gp[k])
    y = g_ref[:, (n - 1) * b : n * b]
    for k in range(n - 2, -1, -1):
        y = g_ref[:, k * b : (k + 1) * b] - mm([y], ge[k])
        g_ref[:, k * b : (k + 1) * b] = y


def apply_matrix(p_ref, before, after, ga, phi, plo, n, b, out):
    phi[:, 0:b], plo[:, 0:b] = split(before)
    phi[:, (n + 1) * b :], plo[:, (n + 1) * b :] = split(after)
    for k in range(n):
        hi, lo = split(p_ref[:, k * b : (k + 1) * b])
        phi[:, (k + 1) * b : (k + 2) * b] = hi
        plo[:, (k + 1) * b : (k + 2) * b] = lo
    for k in range(n):
        window = slice(k * b, (k + 3) * b)
        lhs = jnp.concatenate([phi[:, window], plo[:, window]], axis=1)
        g = ga[k]
        res = jnp.dot(lhs, jnp.concatenate([g, g], axis=0), preferred_element_type=F32)
        out(k, res[:, :b] + res[:, b:])


def setup_kernel(bl, bd, bu, fl, pi, gl, ge, gp, ga, gvw, wt, vb, ts):
    n, b = bd.shape[0], bd.shape[1]
    for k in range(n):
        gl[k] = row(fl[k].T)
        pr = row(pi[k].T)
        gp[k] = pr
        ut = bu[k].T
        ga[k, 0:b] = row(bl[k].T)
        ga[k, b : 2 * b] = row(bd[k].T)
        ga[k, 2 * b :] = row(ut)
        ge[k] = row(mm([ut], pr))
    z = bl[0].T
    v = mm([bu[n - 1].T], gp[n - 1])
    vb[...] = v
    gvw[n - 1, 0:b] = row(v)
    for k in range(n):
        if k:
            z = -mm([z], gl[k])
            v = -mm([v], ge[n - 1 - k])
            gvw[n - 1 - k, 0:b] = row(v)
        ts[k] = mm([z], gp[k])
    w = ts[n - 1]
    gvw[n - 1, b:] = row(w)
    for k in range(n - 2, -1, -1):
        w = ts[k] - mm([w], ge[k])
        gvw[k, b:] = row(w)
    wt[...] = w


def inverse_kernel(wt, vbp, x, a):
    b = wt.shape[0]
    eye = (
        lax.broadcasted_iota(jnp.int32, (b, b), 0) == lax.broadcasted_iota(jnp.int32, (b, b), 1)
    ).astype(F32)
    dot = lambda l, r: jnp.dot(l, r, precision=HIGHEST, preferred_element_type=F32)
    t = dot(vbp[...], wt[...])
    a[...] = eye - t
    near = jnp.sum(t * t) < 0.25
    s = a[...]
    x[...] = jnp.where(near, eye + t, s.T / jnp.sum(s * s))

    def body(carry):
        step, _ = carry
        r = eye - dot(a[...], x[...])
        x[...] = x[...] + dot(x[...], r)
        return step + 1, jnp.sum(r * r)

    lax.while_loop(lambda c: (c[0] < 80) & (c[1] > 1e-8), body, (0, jnp.float32(1.0)))


def columns_to_rows(cols):
    m = cols[0].shape[0]
    lane = lax.broadcasted_iota(jnp.int32, (m, m), 1)
    grid = jnp.zeros((m, m), F32)
    for i, col in enumerate(cols):
        grid = jnp.where(lane == i, col, grid)
    return grid.T[0:8]


def rows_to_columns(rows, count):
    m = rows.shape[1]
    grid = jnp.concatenate([rows, jnp.zeros((m - rows.shape[0], m), F32)], axis=0).T
    return [grid[:, i : i + 1] for i in range(count)]


def first_kernel(rhs, start, before, after, ga, gl, ge, gp, r, g, phi, plo):
    n, b = ga.shape[0], before.shape[1]

    def out(k, value):
        r[:, k * b : (k + 1) * b] = rhs[:, k * b : (k + 1) * b] - value

    apply_matrix(start, before[...], after[...], ga, phi, plo, n, b, out)
    local_solve(r, g, gl, ge, gp, n, b)


def pre_kernel(g, gbp, gtn, wt, vbp, sinv, wtn, sinvn, gvw, p):
    n, b = gvw.shape[0], gvw.shape[1] // 2
    xt = mm([g[:, 0:b] - mm([gbp[...]], row(wt[...]))], row(sinv[...]))
    xtn = mm([gtn[...] - mm([g[:, (n - 1) * b :]], row(wtn[...]))], row(sinvn[...]))
    xb = gbp[...] - mm([xt], row(vbp[...]))
    for k in range(n):
        p[:, k * b : (k + 1) * b] = g[:, k * b : (k + 1) * b] - mm([xtn, xb], gvw[k])


def mapped_kernel(j, *refs):
    p, before, after, ga = refs[:4]
    ks = refs[4 : 5 + j]
    w, prods, phi, plo = refs[5 + j :]
    n, b = ga.shape[0], before.shape[1]
    acc = [None] * (j + 2 + (j == 0))

    def out(k, value):
        w[:, k * b : (k + 1) * b] = value
        vs = [kk[:, k * b : (k + 1) * b] for kk in ks]
        terms = [value * v for v in vs] + [value * value]
        if j == 0:
            terms.append(vs[0] * vs[0])
        for i, t in enumerate(terms):
            acc[i] = t if acc[i] is None else acc[i] + t

    apply_matrix(p, before[...], after[...], ga, phi, plo, n, b, out)
    prods[...] = columns_to_rows([jnp.sum(a, axis=1, keepdims=True) for a in acc])


def scalars(j, sums, norm):
    rows = [sums[i : i + 1] for i in range(j + 2)]
    rows[0] = rows[0] / norm
    if j == 0:
        rows = [rows[0] / norm, rows[1] / norm / norm]
    h = rows[: j + 1]
    square = rows[j + 1]
    for x in h:
        square = square - x * x
    return h, jnp.sqrt(jnp.maximum(square, 0.0) + EPS)


def norm_of(sums):
    return jnp.sqrt(sums[2:3] + EPS)


def stack8(rows):
    m = rows[0].shape[1]
    return jnp.concatenate(rows + [jnp.zeros((8 - len(rows), m), F32)], axis=0)


def orth_kernel(j, *refs):
    first, sums, w = refs[:3]
    ks = refs[3 : 4 + j]
    gl, ge, gp, v, g = refs[4 + j : 9 + j]
    n, b = gl.shape[0], gl.shape[1]
    norm = norm_of(first[...])
    h, length = scalars(j, sums[...], norm)
    rows = [x / length for x in h] + [1.0 / length]
    rows[0] = rows[0] / norm
    if j == 0:
        rows[1] = rows[1] / norm
    cols = rows_to_columns(stack8(rows), j + 2)
    for k in range(n):
        s = slice(k * b, (k + 1) * b)
        value = w[:, s] * cols[j + 1]
        for i in range(j + 1):
            value = value - cols[i] * ks[i][:, s]
        v[:, s] = value
    local_solve(v, g, gl, ge, gp, n, b)


def least_squares(matrix, start_norm):
    total = ITERS
    target = [start_norm] + [jnp.zeros_like(start_norm) for _ in range(total)]
    cos_terms, sin_terms = [], []
    for c in range(total):
        for r in range(c):
            up, low = matrix[r][c], matrix[r + 1][c]
            matrix[r][c] = cos_terms[r] * up + sin_terms[r] * low
            matrix[r + 1][c] = cos_terms[r] * low - sin_terms[r] * up
        up, low = matrix[c][c], matrix[c + 1][c]
        radius = jnp.sqrt(up * up + low * low)
        cos_terms.append(up / radius)
        sin_terms.append(low / radius)
        matrix[c][c] = radius
        target[c + 1] = -sin_terms[c] * target[c]
        target[c] = cos_terms[c] * target[c]
    weights = [None] * total
    for r in range(total - 1, -1, -1):
        part = target[r]
        for c in range(r + 1, total):
            part = part - matrix[r][c] * weights[c]
        weights[r] = part / matrix[r][r]
    return weights


def final_kernel(s0, s1, s2, r, k1, k2, w, p0, p1, p2, start, sol, kry, hess):
    m = r.shape[0]
    zero = jnp.zeros((1, m), F32)
    matrix = [[zero] * ITERS for _ in range(ITERS + 1)]
    norm = norm_of(s0[...])
    for j, s in enumerate((s0, s1, s2)):
        h, length = scalars(j, s[...], norm)
        for i in range(j + 1):
            matrix[i][j] = h[i]
        matrix[j + 1][j] = length
    for i in range(ITERS + 1):
        hess[i] = jnp.concatenate(matrix[i], axis=0)
    last = matrix[3][2]
    rows = [1.0 / norm, matrix[0][2] / last / norm, matrix[1][2] / last, matrix[2][2] / last]
    rows.append(1.0 / last)
    y = least_squares(matrix, norm)
    rows += [y[0] / norm, y[1], y[2]]
    c = rows_to_columns(jnp.concatenate(rows, axis=0), 8)
    step = 128
    for k in range(r.shape[1] // step):
        s = slice(k * step, (k + 1) * step)
        a, u, v = r[:, s], k1[:, s], k2[:, s]
        kry[0, :, s] = a * c[0]
        kry[1, :, s] = u
        kry[2, :, s] = v
        kry[3, :, s] = w[:, s] * c[4] - c[1] * a - c[2] * u - c[3] * v
        sol[:, s] = start[:, s] + c[5] * p0[:, s] + c[6] * p1[:, s] + c[7] * p2[:, s]


def call(body, outs, args, scratch=(), name=None, flops=0):
    vm = pl.BlockSpec(memory_space=pltpu.VMEM)
    size = sum(a.size * a.dtype.itemsize for a in args)
    return pl.pallas_call(
        body,
        name=name,
        out_shape=[jax.ShapeDtypeStruct(s, d) for s, d in outs],
        in_specs=[vm] * len(args),
        out_specs=[vm] * len(outs),
        scratch_shapes=list(scratch),
        cost_estimate=pl.CostEstimate(flops=flops, bytes_accessed=size, transcendentals=0),
    )(*args)


def passed(value, steps):
    count = lax.axis_size("rows")
    first, last = (max(0, -steps), min(count, count - steps))
    return lax.ppermute(value, "rows", [(s, s + steps) for s in range(first, last)])


def local(bl, bd, bu, fl, pi, rhs, start):
    n, b = bd.shape[0], bd.shape[1]
    m, width = rhs.shape
    vec, edge, sq = ((m, width), F32), ((m, b), F32), ((b, b), F32)
    pads = [pltpu.VMEM((m, (n + 2) * b), BF16)] * 2
    before, after = passed(start[:, width - b :], 1), passed(start[:, :b], -1)
    g1, g2, g3 = ((n, b, 2 * b), BF16), ((n, 2 * b, 2 * b), BF16), ((n, 3 * b, 2 * b), BF16)
    gl, ge, gp, ga, gvw, wt, vb = call(
        setup_kernel, [g1, g1, g1, g3, g2, sq, sq], [bl, bd, bu, fl, pi],
        [pltpu.VMEM((n, b, b), F32)], "setup", 2 * n * 8 * 4 * b**3,
    )
    vbp = passed(vb, 1)
    wtn = passed(wt, -1)
    r, g = call(
        first_kernel, [vec, vec], [rhs, start, before, after, ga, gl, ge, gp], pads, "first",
        2 * n * 6 * 4 * b * b * m,
    )
    gbp, gtn = passed(g[:, width - b :], 1), passed(g[:, :b], -1)
    (sinv,) = call(inverse_kernel, [sq], [wt, vbp], [pltpu.VMEM((b, b), F32)], "inverse", 10**8)
    sinvn = passed(sinv, -1)
    ks, ps, sums = [r], [], []
    for j in range(ITERS):
        (p,) = call(
            pre_kernel, [vec], [g, gbp, gtn, wt, vbp, sinv, wtn, sinvn, gvw], (), f"pre{j}",
            2 * n * 2 * 4 * b * b * m,
        )
        ps.append(p)
        before, after = passed(p[:, width - b :], 1), passed(p[:, :b], -1)
        w, prods = call(
            lambda *a, j=j: mapped_kernel(j, *a), [vec, ((8, m), F32)],
            [p, before, after, ga] + ks, pads, f"mapped{j}", 2 * n * 3 * 4 * b * b * m,
        )
        sums.append(lax.psum(prods, "rows"))
        if j < ITERS - 1:
            v, g = call(
                lambda *a, j=j: orth_kernel(j, *a), [vec, vec],
                [sums[0], sums[j], w] + ks + [gl, ge, gp], (), f"orth{j}", 2 * n * 3 * 4 * b * b * m,
            )
            ks.append(v)
            gbp, gtn = passed(g[:, width - b :], 1), passed(g[:, :b], -1)
    return call(
        final_kernel, [vec, ((ITERS + 1, m, width), F32), ((ITERS + 1, ITERS, m), F32)],
        sums + ks + [w] + ps + [start], (), "final", 10**7,
    )


def solution(mesh):
    def run(*args):
        return tuple(local(*args))

    return jax.shard_map(
        run,
        mesh=mesh,
        in_specs=(P("rows", None, None),) * 5 + (P(None, "rows"),) * 2,
        out_specs=(P(None, "rows"), P(None, None, "rows"), P()),
        check_vma=False,
    )
```

```python
import jax
import jax.numpy as jnp
from jax import lax
from jax.experimental import pallas as pl
from jax.experimental.pallas import tpu as pltpu
from jax.sharding import PartitionSpec as P

ITERS = 3
EPS = 1e-06
F32, BF16 = jnp.float32, jnp.bfloat16
HIGHEST = lax.Precision.HIGHEST


def split(x):
    hi = x.astype(BF16)
    return hi, (x - hi.astype(F32)).astype(BF16)


def row(mt):
    return jnp.concatenate(split(mt), axis=1)


def mm(parts, g):
    halves = [split(part) for part in parts]
    lhs = jnp.concatenate([h for h, _ in halves] + [l for _, l in halves], axis=1)
    out = jnp.dot(lhs, jnp.concatenate([g, g], axis=0), preferred_element_type=F32)
    width = out.shape[1] // 2
    return out[:, :width] + out[:, width:]


def local_solve(f_ref, g_ref, gl, ge, gp, n, b):
    z = f_ref[:, 0:b]
    for k in range(n):
        if k:
            z = f_ref[:, k * b : (k + 1) * b] - mm([z], gl[k])
        g_ref[:, k * b : (k + 1) * b] = mm([z], gp[k])
    y = g_ref[:, (n - 1) * b : n * b]
    for k in range(n - 2, -1, -1):
        y = g_ref[:, k * b : (k + 1) * b] - mm([y], ge[k])
        g_ref[:, k * b : (k + 1) * b] = y


def apply_matrix(p_ref, before, after, ga, phi, plo, n, b, out):
    phi[:, 0:b], plo[:, 0:b] = split(before)
    phi[:, (n + 1) * b :], plo[:, (n + 1) * b :] = split(after)
    for k in range(n):
        hi, lo = split(p_ref[:, k * b : (k + 1) * b])
        phi[:, (k + 1) * b : (k + 2) * b] = hi
        plo[:, (k + 1) * b : (k + 2) * b] = lo
    for k in range(n):
        window = slice(k * b, (k + 3) * b)
        lhs = jnp.concatenate([phi[:, window], plo[:, window]], axis=1)
        g = ga[k]
        res = jnp.dot(lhs, jnp.concatenate([g, g], axis=0), preferred_element_type=F32)
        out(k, res[:, :b] + res[:, b:])


def setup_kernel(bl, bd, bu, fl, pi, gl, ge, gp, ga, gvw, wt, vb, ts):
    n, b = bd.shape[0], bd.shape[1]
    for k in range(n):
        gl[k] = row(fl[k].T)
        pr = row(pi[k].T)
        gp[k] = pr
        ut = bu[k].T
        ga[k, 0:b] = row(bl[k].T)
        ga[k, b : 2 * b] = row(bd[k].T)
        ga[k, 2 * b :] = row(ut)
        ge[k] = row(mm([ut], pr))
    z = bl[0].T
    v = mm([bu[n - 1].T], gp[n - 1])
    vb[...] = v
    gvw[n - 1, 0:b] = row(v)
    for k in range(n):
        if k:
            z = -mm([z], gl[k])
            v = -mm([v], ge[n - 1 - k])
            gvw[n - 1 - k, 0:b] = row(v)
        ts[k] = mm([z], gp[k])
    w = ts[n - 1]
    gvw[n - 1, b:] = row(w)
    for k in range(n - 2, -1, -1):
        w = ts[k] - mm([w], ge[k])
        gvw[k, b:] = row(w)
    wt[...] = w


def inverse_kernel(wt, vbp, x, a):
    b = wt.shape[0]
    eye = (
        lax.broadcasted_iota(jnp.int32, (b, b), 0) == lax.broadcasted_iota(jnp.int32, (b, b), 1)
    ).astype(F32)
    dot = lambda l, r: jnp.dot(l, r, precision=HIGHEST, preferred_element_type=F32)
    t = dot(vbp[...], wt[...])
    a[...] = eye - t
    near = jnp.sum(t * t) < 0.25
    s = a[...]
    x[...] = jnp.where(near, eye + t, s.T / jnp.sum(s * s))

    def body(carry):
        step, _ = carry
        r = eye - dot(a[...], x[...])
        x[...] = x[...] + dot(x[...], r)
        return step + 1, jnp.sum(r * r)

    lax.while_loop(lambda c: (c[0] < 80) & (c[1] > 1e-8), body, (0, jnp.float32(1.0)))


def columns_to_rows(cols):
    m = cols[0].shape[0]
    lane = lax.broadcasted_iota(jnp.int32, (m, m), 1)
    grid = jnp.zeros((m, m), F32)
    for i, col in enumerate(cols):
        grid = jnp.where(lane == i, col, grid)
    return grid.T[0:8]


def rows_to_columns(rows, count):
    m = rows.shape[1]
    grid = jnp.concatenate([rows, jnp.zeros((m - rows.shape[0], m), F32)], axis=0).T
    return [grid[:, i : i + 1] for i in range(count)]


def first_kernel(rhs, start, before, after, ga, gl, ge, gp, r, g, phi, plo):
    n, b = ga.shape[0], before.shape[1]

    def out(k, value):
        r[:, k * b : (k + 1) * b] = rhs[:, k * b : (k + 1) * b] - value

    apply_matrix(start, before[...], after[...], ga, phi, plo, n, b, out)
    local_solve(r, g, gl, ge, gp, n, b)


def pre_kernel(g, gbp, gtn, wt, vbp, sinv, wtn, sinvn, gvw, p):
    n, b = gvw.shape[0], gvw.shape[1] // 2
    xt = mm([g[:, 0:b] - mm([gbp[...]], row(wt[...]))], row(sinv[...]))
    xtn = mm([gtn[...] - mm([g[:, (n - 1) * b :]], row(wtn[...]))], row(sinvn[...]))
    xb = gbp[...] - mm([xt], row(vbp[...]))
    for k in range(n):
        p[:, k * b : (k + 1) * b] = g[:, k * b : (k + 1) * b] - mm([xtn, xb], gvw[k])


def mapped_kernel(j, *refs):
    p, before, after, ga = refs[:4]
    ks = refs[4 : 5 + j]
    w, prods, phi, plo = refs[5 + j :]
    n, b = ga.shape[0], before.shape[1]
    acc = [None] * (j + 2 + (j == 0))

    def out(k, value):
        w[:, k * b : (k + 1) * b] = value
        vs = [kk[:, k * b : (k + 1) * b] for kk in ks]
        terms = [value * v for v in vs] + [value * value]
        if j == 0:
            terms.append(vs[0] * vs[0])
        for i, t in enumerate(terms):
            acc[i] = t if acc[i] is None else acc[i] + t

    apply_matrix(p, before[...], after[...], ga, phi, plo, n, b, out)
    prods[...] = columns_to_rows([jnp.sum(a, axis=1, keepdims=True) for a in acc])


def scalars(j, sums, norm):
    rows = [sums[i : i + 1] for i in range(j + 2)]
    rows[0] = rows[0] / norm
    if j == 0:
        rows = [rows[0] / norm, rows[1] / norm / norm]
    h = rows[: j + 1]
    square = rows[j + 1]
    for x in h:
        square = square - x * x
    return h, jnp.sqrt(jnp.maximum(square, 0.0) + EPS)


def norm_of(sums):
    return jnp.sqrt(sums[2:3] + EPS)


def stack8(rows):
    m = rows[0].shape[1]
    return jnp.concatenate(rows + [jnp.zeros((8 - len(rows), m), F32)], axis=0)


def orth_kernel(j, *refs):
    first, sums, w = refs[:3]
    ks = refs[3 : 4 + j]
    gl, ge, gp, v, g = refs[4 + j : 9 + j]
    n, b = gl.shape[0], gl.shape[1]
    norm = norm_of(first[...])
    h, length = scalars(j, sums[...], norm)
    rows = [x / length for x in h] + [1.0 / length]
    rows[0] = rows[0] / norm
    if j == 0:
        rows[1] = rows[1] / norm
    cols = rows_to_columns(stack8(rows), j + 2)
    for k in range(n):
        s = slice(k * b, (k + 1) * b)
        value = w[:, s] * cols[j + 1]
        for i in range(j + 1):
            value = value - cols[i] * ks[i][:, s]
        v[:, s] = value
    local_solve(v, g, gl, ge, gp, n, b)


def least_squares(matrix, start_norm):
    total = ITERS
    target = [start_norm] + [jnp.zeros_like(start_norm) for _ in range(total)]
    cos_terms, sin_terms = [], []
    for c in range(total):
        for r in range(c):
            up, low = matrix[r][c], matrix[r + 1][c]
            matrix[r][c] = cos_terms[r] * up + sin_terms[r] * low
            matrix[r + 1][c] = cos_terms[r] * low - sin_terms[r] * up
        up, low = matrix[c][c], matrix[c + 1][c]
        radius = jnp.sqrt(up * up + low * low)
        cos_terms.append(up / radius)
        sin_terms.append(low / radius)
        matrix[c][c] = radius
        target[c + 1] = -sin_terms[c] * target[c]
        target[c] = cos_terms[c] * target[c]
    weights = [None] * total
    for r in range(total - 1, -1, -1):
        part = target[r]
        for c in range(r + 1, total):
            part = part - matrix[r][c] * weights[c]
        weights[r] = part / matrix[r][r]
    return weights


def final_kernel(s0, s1, s2, r, k1, k2, w, p0, p1, p2, start, sol, kry, hess):
    m = r.shape[0]
    zero = jnp.zeros((1, m), F32)
    matrix = [[zero] * ITERS for _ in range(ITERS + 1)]
    norm = norm_of(s0[...])
    for j, s in enumerate((s0, s1, s2)):
        h, length = scalars(j, s[...], norm)
        for i in range(j + 1):
            matrix[i][j] = h[i]
        matrix[j + 1][j] = length
    for i in range(ITERS + 1):
        hess[i] = jnp.concatenate(matrix[i], axis=0)
    last = matrix[3][2]
    rows = [1.0 / norm, matrix[0][2] / last / norm, matrix[1][2] / last, matrix[2][2] / last]
    rows.append(1.0 / last)
    y = least_squares(matrix, norm)
    rows += [y[0] / norm, y[1], y[2]]
    c = rows_to_columns(jnp.concatenate(rows, axis=0), 8)
    step = 128
    for k in range(r.shape[1] // step):
        s = slice(k * step, (k + 1) * step)
        a, u, v = r[:, s], k1[:, s], k2[:, s]
        kry[0, :, s] = a * c[0]
        kry[1, :, s] = u
        kry[2, :, s] = v
        kry[3, :, s] = w[:, s] * c[4] - c[1] * a - c[2] * u - c[3] * v
        sol[:, s] = start[:, s] + c[5] * p0[:, s] + c[6] * p1[:, s] + c[7] * p2[:, s]


def call(body, outs, args, scratch=(), name=None, flops=0):
    vm = pl.BlockSpec(memory_space=pltpu.VMEM)
    size = sum(a.size * a.dtype.itemsize for a in args)
    return pl.pallas_call(
        body,
        name=name,
        out_shape=[jax.ShapeDtypeStruct(s, d) for s, d in outs],
        in_specs=[vm] * len(args),
        out_specs=[vm] * len(outs),
        scratch_shapes=list(scratch),
        cost_estimate=pl.CostEstimate(flops=flops, bytes_accessed=size, transcendentals=0),
    )(*args)


def exchange_kernel(up, down, before, after, send, recv):
    me, count = lax.axis_index("rows"), lax.axis_size("rows")
    b = before.shape[1]
    barrier = pltpu.get_barrier_semaphore()
    inner, outer = me > 0, me < count - 1

    def copy(src, dst, i, device):
        return pltpu.make_async_remote_copy(
            src_ref=src, dst_ref=dst, send_sem=send.at[i], recv_sem=recv.at[i],
            device_id=(device,), device_id_type=pl.DeviceIdType.MESH,
        )

    to_next = lambda: copy(up.at[:, up.shape[1] - b :], before, 0, me + 1)
    to_prev = lambda: copy(down.at[:, 0:b], after, 1, me - 1)

    @pl.when(inner)
    def _():
        pl.semaphore_signal(barrier, 1, device_id=(me - 1,), device_id_type=pl.DeviceIdType.MESH)

    @pl.when(outer)
    def _():
        pl.semaphore_signal(barrier, 1, device_id=(me + 1,), device_id_type=pl.DeviceIdType.MESH)

    @pl.when(inner & outer)
    def _():
        pl.semaphore_wait(barrier, 2)

    @pl.when(~(inner & outer))
    def _():
        pl.semaphore_wait(barrier, 1)

    @pl.when(outer)
    def _():
        to_next().start()

    @pl.when(inner)
    def _():
        to_prev().start()

    @pl.when(me == 0)
    def _():
        before[...] = jnp.zeros_like(before)

    @pl.when(me == count - 1)
    def _():
        after[...] = jnp.zeros_like(after)

    @pl.when(outer)
    def _():
        to_next().wait_send()
        copy(down.at[:, 0:b], after, 1, me + 1).wait_recv()

    @pl.when(inner)
    def _():
        to_prev().wait_send()
        copy(up.at[:, up.shape[1] - b :], before, 0, me - 1).wait_recv()


def exchange(up, down, b, number):
    shape = jax.ShapeDtypeStruct((up.shape[0], b), F32)
    return pl.pallas_call(
        exchange_kernel,
        name="exchange",
        out_shape=[shape, shape],
        in_specs=[pl.BlockSpec(memory_space=pl.ANY)] * 2,
        out_specs=[pl.BlockSpec(memory_space=pltpu.VMEM)] * 2,
        scratch_shapes=[pltpu.SemaphoreType.DMA((2,))] * 2,
        compiler_params=pltpu.CompilerParams(collective_id=number, has_side_effects=True),
    )(up, down)


def reduce_kernel(x, out, slots, send, recv):
    me, count = lax.axis_index("rows"), lax.axis_size("rows")
    barrier = pltpu.get_barrier_semaphore()

    def copy(k, slot, device):
        return pltpu.make_async_remote_copy(
            src_ref=x, dst_ref=slots.at[slot], send_sem=send.at[k], recv_sem=recv.at[slot],
            device_id=(device,), device_id_type=pl.DeviceIdType.MESH,
        )

    @pl.loop(1, count)
    def _(k):
        pl.semaphore_signal(
            barrier, 1, device_id=(lax.rem(me + k, count),), device_id_type=pl.DeviceIdType.MESH
        )

    pl.semaphore_wait(barrier, count - 1)

    @pl.loop(1, count)
    def _(k):
        copy(k, me, lax.rem(me + k, count)).start()

    slots[me] = x[...]

    @pl.loop(1, count)
    def _(k):
        other = lax.rem(me + k, count)
        copy(k, me, other).wait_send()
        copy(k, other, other).wait_recv()

    total = slots[0]
    for i in range(1, count):
        total = total + slots[i]
    out[...] = total


def all_sum(x):
    count = lax.axis_size("rows")
    vm = pl.BlockSpec(memory_space=pltpu.VMEM)
    return pl.pallas_call(
        reduce_kernel,
        name="allsum",
        out_shape=jax.ShapeDtypeStruct(x.shape, F32),
        in_specs=[vm],
        out_specs=vm,
        scratch_shapes=[pltpu.VMEM((count,) + x.shape, F32)]
        + [pltpu.SemaphoreType.DMA((count,))] * 2,
        compiler_params=pltpu.CompilerParams(collective_id=3, has_side_effects=True),
    )(x)


def local(bl, bd, bu, fl, pi, rhs, start):
    n, b = bd.shape[0], bd.shape[1]
    m, width = rhs.shape
    vec, edge, sq = ((m, width), F32), ((m, b), F32), ((b, b), F32)
    pads = [pltpu.VMEM((m, (n + 2) * b), BF16)] * 2
    before, after = exchange(start, start, b, 1)
    g1, g2, g3 = ((n, b, 2 * b), BF16), ((n, 2 * b, 2 * b), BF16), ((n, 3 * b, 2 * b), BF16)
    gl, ge, gp, ga, gvw, wt, vb = call(
        setup_kernel, [g1, g1, g1, g3, g2, sq, sq], [bl, bd, bu, fl, pi],
        [pltpu.VMEM((n, b, b), F32)], "setup", 2 * n * 8 * 4 * b**3,
    )
    vbp, wtn = exchange(vb, wt, b, 2)
    r, g = call(
        first_kernel, [vec, vec], [rhs, start, before, after, ga, gl, ge, gp], pads, "first",
        2 * n * 6 * 4 * b * b * m,
    )
    gbp, gtn = exchange(g, g, b, 1)
    (sinv,) = call(inverse_kernel, [sq], [wt, vbp], [pltpu.VMEM((b, b), F32)], "inverse", 10**8)
    _, sinvn = exchange(sinv, sinv, b, 2)
    ks, ps, sums = [r], [], []
    for j in range(ITERS):
        (p,) = call(
            pre_kernel, [vec], [g, gbp, gtn, wt, vbp, sinv, wtn, sinvn, gvw], (), f"pre{j}",
            2 * n * 2 * 4 * b * b * m,
        )
        ps.append(p)
        before, after = exchange(p, p, b, 1)
        w, prods = call(
            lambda *a, j=j: mapped_kernel(j, *a), [vec, ((8, m), F32)],
            [p, before, after, ga] + ks, pads, f"mapped{j}", 2 * n * 3 * 4 * b * b * m,
        )
        sums.append(all_sum(prods))
        if j < ITERS - 1:
            v, g = call(
                lambda *a, j=j: orth_kernel(j, *a), [vec, vec],
                [sums[0], sums[j], w] + ks + [gl, ge, gp], (), f"orth{j}", 2 * n * 3 * 4 * b * b * m,
            )
            ks.append(v)
            gbp, gtn = exchange(g, g, b, 1)
    return call(
        final_kernel, [vec, ((ITERS + 1, m, width), F32), ((ITERS + 1, ITERS, m), F32)],
        sums + ks + [w] + ps + [start], (), "final", 10**7,
    )


def solution(mesh):
    def run(*args):
        return tuple(local(*args))

    return jax.shard_map(
        run,
        mesh=mesh,
        in_specs=(P("rows", None, None),) * 5 + (P(None, "rows"),) * 2,
        out_specs=(P(None, "rows"), P(None, None, "rows"), P()),
        check_vma=False,
    )
```
